32 devices in a mesh: vpair: 4 (over y, x), rank: 8 (over z, core).
Axes of the slice: x: 2, y: 2, z: 4, core: 2. Of those that a mesh axis runs over, the one named last changes fastest.
Arguments:
- amplitudes: bfloat16 [8, 1200, 1200], P(None, 'vpair', 'rank'), may hold values from -6 to 6
- factors: bfloat16 [1200, 8192], P('vpair', 'rank'), may hold values from -0.1875 to 0.1875
- kernel: bfloat16 [8192, 8192], P('vpair', 'rank'), may hold values from -0.875 to 0.875
- other_terms: float32 [8, 1200, 1200], P(None, 'vpair'), may hold values from -6 to 6
- virt_energy: float32 [1200], replicated, may hold values from 0.2 to 4
- pair_energy: float32 [8], replicated, may hold values from -3 to -0.5
Outputs:
- residual: float32 [8, 1200, 1200], P(None, 'vpair')
- update_rms: float32 [], replicated
The draws below stay inside these ranges and needn't reach their ends.
All inputs are finite; a program needn't handle non-finite values.
Results may differ from the reference program's by a relative error of at most 0.0035.
Values may be sent and summed in bfloat16 or wider, within the bound.
A program may use at most 192 MiB of HBM per device.

```python
import jax
import jax.numpy as jnp
from jax import lax

NVIR = 1200
NTHC = 8192
PAIRS = 8


def draw_virt_energy(key, part):
    jitter = jax.random.uniform(key, (NVIR,), jnp.float32)
    spread = (jnp.arange(NVIR, dtype=jnp.float32) + jitter) / NVIR
    return 0.2 + 3.8 * spread


def block_levels(rng, dims, split, smallest, largest):
    gain = 1.0
    for axis_at, parts in split:
        heights = jax.random.uniform(jax.random.fold_in(jax.random.fold_in(rng, 6), axis_at), (parts,), jnp.float32, smallest / len(split), largest / len(split))
        gain = gain * jnp.repeat(jnp.exp(heights), dims[axis_at] // parts).reshape((-1,) + (1,) * (len(dims) - 1 - axis_at))
    return gain


def centred(rng, shape, scale, limit, cuts=(), held_as=jnp.bfloat16):
    drawn = scale * jax.random.normal(rng, shape, jnp.float32)
    if cuts:
        drawn = drawn * block_levels(rng, shape, cuts, -0.22, 0.18)
    return jnp.clip(drawn, -limit, limit).astype(held_as)


def setup_inputs(seed: int = 0) -> dict:
    keys = jax.random.split(jax.random.key(seed), 7)
    amplitudes = centred(keys[0], (PAIRS, NVIR, NVIR), 1.0, 6.0, ((1, 4), (2, 8)))
    factors = centred(keys[1], (NVIR, NTHC), NVIR ** -0.5, 0.1875, ((0, 4), (1, 8)))
    kernel = centred(keys[2], (NTHC, NTHC), (NTHC * NTHC // (NVIR * NVIR)) ** -0.5, 0.875, ((0, 4), (1, 8)))
    other_terms = centred(keys[3], (PAIRS, NVIR, NVIR), 1.0, 6.0, ((1, 4),), jnp.float32)
    virt_energy = draw_virt_energy(jax.random.fold_in(keys[6], 71), 0)
    pair_energy = jnp.clip(jax.random.uniform(keys[5], (PAIRS,), jnp.float32, -3.0, -0.5), -3.0, -0.5)
    return dict(amplitudes=amplitudes, factors=factors, kernel=kernel, other_terms=other_terms, virt_energy=virt_energy, pair_energy=pair_energy)


epsilon = 1e-06

def reference(amplitudes, factors, kernel, other_terms, virt_energy, pair_energy):
    kernel_wide = kernel.astype(jnp.float32)

    def one_pair(operands):
        amplitude, other_block, pair_value = operands
        first_half = jnp.dot(amplitude, factors, preferred_element_type=jnp.float32).astype(jnp.bfloat16)
        coupled = jnp.dot(factors.T, first_half, preferred_element_type=jnp.float32)
        weighted = (kernel_wide * coupled).astype(jnp.bfloat16)
        back_half = jnp.dot(factors, weighted, preferred_element_type=jnp.float32).astype(jnp.bfloat16)
        ladder = jnp.dot(back_half, factors.T, preferred_element_type=jnp.float32)
        residual = other_block + ladder
        denominator = virt_energy[:, None] + virt_energy[None, :] - pair_value
        update = residual / denominator
        return (residual, jnp.sum(update * update))
    residual, squares = lax.map(one_pair, (amplitudes, other_terms, pair_energy))
    update_rms = jnp.sqrt(jnp.sum(squares) / (PAIRS * NVIR * NVIR) + epsilon)
    return (residual, update_rms)
```

```python
import functools

import jax
import jax.numpy as jnp
from jax import lax
from jax.experimental import pallas as pl
from jax.experimental.pallas import tpu as pltpu
from jax.sharding import PartitionSpec as P

epsilon = 1e-06


def shards(amplitudes, factors, kernel, other_terms, virt_energy, pair_energy):
    vpair_count = lax.axis_size("vpair")
    pair_count = amplitudes.shape[0]
    row_block = amplitudes.shape[1]
    col_block = amplitudes.shape[2]
    virt_count = row_block * vpair_count
    right_block = kernel.shape[1]
    factor_rows = lax.all_gather(factors, "rank", axis=1, tiled=True)
    factor_full = lax.all_gather(factor_rows, "vpair", axis=0, tiled=True)
    factor_cols = lax.dynamic_slice_in_dim(
        factor_full, lax.axis_index("rank") * right_block, right_block, 1
    )
    half_done = jnp.einsum(
        "ons,sh->onh",
        lax.all_gather(amplitudes, "rank", axis=2, tiled=True),
        factor_cols,
        preferred_element_type=jnp.float32,
    ).astype(jnp.bfloat16)
    kernel_sub = lax.all_to_all(kernel, "vpair", split_axis=1, concat_axis=0, tiled=True).astype(
        jnp.float32
    )
    coupled = jnp.einsum(
        "cp,icq->ipq",
        factor_full,
        lax.all_to_all(half_done, "vpair", split_axis=2, concat_axis=1, tiled=True),
        preferred_element_type=jnp.float32,
    )
    weighted = (kernel_sub[None] * coupled).astype(jnp.bfloat16)
    ladder_half = jnp.einsum(
        "ap,ipq->iaq", factor_full, weighted, preferred_element_type=jnp.float32
    ).astype(jnp.bfloat16)
    back_half = lax.all_to_all(ladder_half, "vpair", split_axis=1, concat_axis=2, tiled=True)
    partial_value = jnp.einsum(
        "iaq,bq->iab", back_half, factor_cols, preferred_element_type=jnp.float32
    )
    row_energy = lax.dynamic_slice_in_dim(
        virt_energy, lax.axis_index("vpair") * row_block, row_block, 0
    )
    ladder_share = lax.psum_scatter(partial_value, "rank", scatter_dimension=2, tiled=True)
    col_start = lax.axis_index("rank") * col_block
    own_terms = lax.dynamic_slice_in_dim(other_terms, col_start, col_block, 2)
    part_residual = own_terms + ladder_share
    col_energy = lax.dynamic_slice_in_dim(virt_energy, col_start, col_block, 0)
    denominator = row_energy[None, :, None] + col_energy[None, None, :] - pair_energy[:, None, None]
    update = part_residual / denominator
    squares = lax.psum(jnp.sum(update * update), ("vpair", "rank"))
    residual = lax.all_gather(part_residual, "rank", axis=2, tiled=True)
    update_rms = jnp.sqrt(squares / (pair_count * virt_count * virt_count) + epsilon)
    return (residual, update_rms)


def middle_kernel(
    zs, own_ref, half_ref, kern_ref, out_ref, gath_ref, fbuf, fturn, acc, mine_sem, load_sem, recv, s1, s2, s3
):
    v = lax.axis_index("vpair")
    r = lax.axis_index("rank")
    y, x = v // 2, v % 2
    z, core = r // 2, r % 2
    vx, vy, vd = y * 2 + 1 - x, (1 - y) * 2 + x, (1 - y) * 2 + 1 - x
    mate = z * 2 + 1 - core
    pairs, rows, cols = acc.shape
    depth = own_ref.shape[1]

    def rank_at(k):
        return ((z + k) % zs) * 2 + core

    barrier = pltpu.get_barrier_semaphore()
    peers = [(v, rank_at(k)) for k in range(1, zs)] + [(vx, r), (vy, r), (v, mate)]
    for peer in peers:
        pl.semaphore_signal(barrier, inc=1, device_id=peer, device_id_type=pl.DeviceIdType.MESH)
    pl.semaphore_wait(barrier, len(peers))

    started = []

    def send(src, rr, vv, sem, to):
        copy = pltpu.make_async_remote_copy(
            src_ref=src,
            dst_ref=gath_ref.at[rr, vv],
            send_sem=sem,
            recv_sem=recv.at[rr, vv],
            device_id=to,
            device_id_type=pl.DeviceIdType.MESH,
        )
        copy.start()
        started.append(copy)

    def arrived(rr, vv):
        pltpu.make_async_copy(gath_ref.at[rr, vv], gath_ref.at[rr, vv], recv.at[rr, vv]).wait()

    send(own_ref, r, v, s2.at[0, 0], (vx, r))
    send(own_ref, r, v, s2.at[0, 1], (vy, r))
    for k in range(1, zs):
        send(own_ref, r, v, s1.at[k], (v, rank_at(k)))
    send(own_ref, r, v, s3.at[0, 0], (v, mate))

    def spread(k):
        rr = rank_at(k)
        arrived(rr, v)
        shard = gath_ref.at[rr, v]
        send(shard, rr, v, s2.at[k, 0], (vx, r))
        send(shard, rr, v, s2.at[k, 1], (vy, r))
        send(shard, rr, v, s3.at[k, 0], (v, mate))

    def relay(k):
        rr = rank_at(k)
        odd = (rr // 2) % 2
        arrived(rr, vx)
        arrived(rr, vy)
        via = (y + odd * (1 - 2 * y)) * 2 + x + (1 - odd) * (1 - 2 * x)
        to = (y + (1 - odd) * (1 - 2 * y)) * 2 + x + odd * (1 - 2 * x)
        send(gath_ref.at[rr, via], rr, via, s2.at[k, 2], (to, r))
        send(gath_ref.at[rr, vx], rr, vx, s3.at[k, 1], (v, mate))
        send(gath_ref.at[rr, vy], rr, vy, s3.at[k, 2], (v, mate))

    def finish(k):
        rr = rank_at(k)
        arrived(rr, vd)
        send(gath_ref.at[rr, vd], rr, vd, s3.at[k, 3], (v, mate))

    def compute(slot, rr, first):
        start = pl.multiple_of(rr * depth, depth)

        @pl.loop(0, depth // 128)
        def _(c):
            piece = fbuf[slot, :, :, pl.ds(pl.multiple_of(c * 128, 128), 128)].reshape(rows, 128)
            fturn[pl.ds(pl.multiple_of(c * 128, 128), 128), :] = piece.T

        @pl.loop(0, pairs)
        def _(i):
            half = half_ref[:, i].reshape(rows, cols)
            coupled = jnp.dot(fturn[...], half, preferred_element_type=jnp.float32)
            weight = kern_ref[pl.ds(start, depth), :].astype(jnp.float32)
            weighted = (weight * coupled).astype(jnp.bfloat16)
            term = jnp.dot(
                fbuf[slot].reshape(rows, depth), weighted, preferred_element_type=jnp.float32
            )
            if first:
                acc[i] = term
            else:
                acc[i] += term

    def fetch(slot, rr):
        for j in range(4):
            pltpu.make_async_copy(gath_ref.at[rr, j], fbuf.at[slot, j], load_sem.at[slot, j]).start()

    def fetched(slot, rr):
        for j in range(4):
            pltpu.make_async_copy(gath_ref.at[rr, j], fbuf.at[slot, j], load_sem.at[slot, j]).wait()

    stage = fbuf.at[1, 0]
    into = pltpu.make_async_copy(own_ref, stage, mine_sem.at[0])
    into.start()
    into.wait()
    back = pltpu.make_async_copy(stage, gath_ref.at[r, v], mine_sem.at[1])
    back.start()
    back.wait()

    relay(0)
    spread(1)
    finish(0)
    fetch(0, r)
    relay(1)
    fetched(0, r)
    compute(0, r, True)
    for k in range(zs):
        other = ((z + k) % zs) * 2 + 1 - core
        if k + 2 < zs:
            spread(k + 2)
        for at in (v, vx, vy, vd):
            arrived(other, at)
        fetch(1, other)
        if k + 1 < zs:
            finish(k + 1)
            fetch(0, rank_at(k + 1))
        fetched(1, other)
        compute(1, other, False)
        if k + 1 < zs:
            if k + 2 < zs:
                relay(k + 2)
            fetched(0, rank_at(k + 1))
            compute(0, rank_at(k + 1), False)
    for i in range(pairs):
        out_ref[:, i] = acc[i].reshape(4, rows // 4, cols).astype(jnp.bfloat16)
    for copy in started:
        copy.wait_send()


def ladder_middle(factors_pad, half_sub, kernel_sub, rank_count):
    count, pairs, block, cols = half_sub.shape
    depth = factors_pad.shape[1]
    rows = count * block
    points = kernel_sub.shape[0]
    zs = rank_count // 2
    hbm = pl.BlockSpec(memory_space=pl.ANY)
    vmem = pl.BlockSpec(memory_space=pltpu.VMEM)
    return pl.pallas_call(
        functools.partial(middle_kernel, zs),
        out_shape=(
            jax.ShapeDtypeStruct((count, pairs, block, cols), jnp.bfloat16),
            jax.ShapeDtypeStruct((rank_count, count, block, depth), jnp.bfloat16),
        ),
        in_specs=[hbm, vmem, vmem],
        out_specs=(vmem, hbm),
        scratch_shapes=[
            pltpu.VMEM((2, count, block, depth), jnp.bfloat16),
            pltpu.VMEM((depth, rows), jnp.bfloat16),
            pltpu.VMEM((pairs, rows, cols), jnp.float32),
            pltpu.SemaphoreType.DMA((2,)),
            pltpu.SemaphoreType.DMA((2, count)),
            pltpu.SemaphoreType.DMA((rank_count, count)),
            pltpu.SemaphoreType.DMA((zs,)),
            pltpu.SemaphoreType.DMA((zs, 3)),
            pltpu.SemaphoreType.DMA((zs, 4)),
        ],
        compiler_params=pltpu.CompilerParams(
            collective_id=0, has_side_effects=True, vmem_limit_bytes=60 * 1024 * 1024
        ),
        cost_estimate=pl.CostEstimate(
            flops=4 * pairs * points * rows * cols, bytes_accessed=4 * points * rows, transcendentals=0
        ),
    )(factors_pad, half_sub, kernel_sub)


def fast_shards(amplitudes, factors, kernel, other_terms, virt_energy, pair_energy):
    vpair_count = lax.axis_size("vpair")
    rank_count = lax.axis_size("rank")
    pair_count, row_block, _ = amplitudes.shape
    virt_count = row_block * vpair_count
    right_block = kernel.shape[1]
    cols = right_block // vpair_count
    block = -(-row_block // 64) * 64
    factor_cols = lax.all_gather(factors, "vpair", axis=0, tiled=False)
    amps = lax.all_gather(amplitudes, "rank", axis=2, tiled=True)
    kernel_sub = lax.all_to_all(kernel, "vpair", split_axis=1, concat_axis=0, tiled=True)
    factor_cols = factor_cols.reshape(virt_count, right_block)
    half_done = jnp.einsum(
        "ons,sh->onh", amps, factor_cols, preferred_element_type=jnp.float32
    ).astype(jnp.bfloat16)
    half_done = jnp.pad(half_done, ((0, 0), (0, block - row_block), (0, 0)))
    half_done = half_done.reshape(pair_count, block, vpair_count, cols).transpose(2, 0, 1, 3)
    half_sub = lax.all_to_all(half_done, "vpair", split_axis=0, concat_axis=0, tiled=True)
    factors_pad = jnp.pad(factors, ((0, block - row_block), (0, 0)))
    back, _ = ladder_middle(factors_pad, half_sub, kernel_sub, rank_count)
    back = lax.all_to_all(back, "vpair", split_axis=0, concat_axis=0, tiled=True)
    back = back[:, :, :row_block]
    partial_value = jnp.einsum(
        "viaq,bvq->iab",
        back,
        factor_cols.reshape(virt_count, vpair_count, cols),
        preferred_element_type=jnp.float32,
    )
    ladder_own = lax.psum_scatter(partial_value, "rank", scatter_dimension=0, tiled=True)
    ladder = lax.all_gather(ladder_own.astype(jnp.bfloat16), "rank", axis=0, tiled=True)
    own = ladder_own.shape[0]
    start = lax.axis_index("rank") * own
    row_energy = lax.dynamic_slice_in_dim(
        virt_energy, lax.axis_index("vpair") * row_block, row_block, 0
    )
    own_terms = lax.dynamic_slice_in_dim(other_terms, start, own, 0)
    own_pairs = lax.dynamic_slice_in_dim(pair_energy, start, own, 0)
    denominator = row_energy[None, :, None] + virt_energy[None, None, :] - own_pairs[:, None, None]
    update = (own_terms + ladder_own) / denominator
    squares = lax.psum(jnp.sum(update * update), ("vpair", "rank"))
    residual = other_terms + ladder.astype(jnp.float32)
    update_rms = jnp.sqrt(squares / (pair_count * virt_count * virt_count) + epsilon)
    return (residual, update_rms)


def pick(amplitudes, factors, kernel, other_terms, virt_energy, pair_energy):
    vpair_count = lax.axis_size("vpair")
    rank_count = lax.axis_size("rank")
    fits = (
        vpair_count == 4
        and rank_count % 2 == 0
        and amplitudes.shape[0] % rank_count == 0
        and kernel.shape[1] % (128 * vpair_count) == 0
    )
    body = fast_shards if fits else shards
    return body(amplitudes, factors, kernel, other_terms, virt_energy, pair_energy)


def solution(mesh):
    placed = (
        P(None, "vpair", "rank"),
        P("vpair", "rank"),
        P("vpair", "rank"),
        P(None, "vpair", None),
        P(),
        P(),
    )
    return jax.shard_map(
        pick, mesh=mesh, in_specs=placed, out_specs=(P(None, "vpair", None), P()), check_vma=False
    )
```

```python
import functools

import jax
import jax.numpy as jnp
from jax import lax
from jax.experimental import pallas as pl
from jax.experimental.pallas import tpu as pltpu
from jax.sharding import PartitionSpec as P

epsilon = 1e-06


def shards(amplitudes, factors, kernel, other_terms, virt_energy, pair_energy):
    vpair_count = lax.axis_size("vpair")
    pair_count = amplitudes.shape[0]
    row_block = amplitudes.shape[1]
    col_block = amplitudes.shape[2]
    virt_count = row_block * vpair_count
    right_block = kernel.shape[1]
    factor_rows = lax.all_gather(factors, "rank", axis=1, tiled=True)
    factor_full = lax.all_gather(factor_rows, "vpair", axis=0, tiled=True)
    factor_cols = lax.dynamic_slice_in_dim(
        factor_full, lax.axis_index("rank") * right_block, right_block, 1
    )
    half_done = jnp.einsum(
        "ons,sh->onh",
        lax.all_gather(amplitudes, "rank", axis=2, tiled=True),
        factor_cols,
        preferred_element_type=jnp.float32,
    ).astype(jnp.bfloat16)
    kernel_sub = lax.all_to_all(kernel, "vpair", split_axis=1, concat_axis=0, tiled=True).astype(
        jnp.float32
    )
    coupled = jnp.einsum(
        "cp,icq->ipq",
        factor_full,
        lax.all_to_all(half_done, "vpair", split_axis=2, concat_axis=1, tiled=True),
        preferred_element_type=jnp.float32,
    )
    weighted = (kernel_sub[None] * coupled).astype(jnp.bfloat16)
    ladder_half = jnp.einsum(
        "ap,ipq->iaq", factor_full, weighted, preferred_element_type=jnp.float32
    ).astype(jnp.bfloat16)
    back_half = lax.all_to_all(ladder_half, "vpair", split_axis=1, concat_axis=2, tiled=True)
    partial_value = jnp.einsum(
        "iaq,bq->iab", back_half, factor_cols, preferred_element_type=jnp.float32
    )
    row_energy = lax.dynamic_slice_in_dim(
        virt_energy, lax.axis_index("vpair") * row_block, row_block, 0
    )
    ladder_share = lax.psum_scatter(partial_value, "rank", scatter_dimension=2, tiled=True)
    col_start = lax.axis_index("rank") * col_block
    own_terms = lax.dynamic_slice_in_dim(other_terms, col_start, col_block, 2)
    part_residual = own_terms + ladder_share
    col_energy = lax.dynamic_slice_in_dim(virt_energy, col_start, col_block, 0)
    denominator = row_energy[None, :, None] + col_energy[None, None, :] - pair_energy[:, None, None]
    update = part_residual / denominator
    squares = lax.psum(jnp.sum(update * update), ("vpair", "rank"))
    residual = lax.all_gather(part_residual, "rank", axis=2, tiled=True)
    update_rms = jnp.sqrt(squares / (pair_count * virt_count * virt_count) + epsilon)
    return (residual, update_rms)


def middle_kernel(
    zs, own_ref, half_ref, kern_ref, out_ref, gath_ref, fbuf, fturn, acc, mine_sem, load_sem, recv, s1, s2, s3
):
    v = lax.axis_index("vpair")
    r = lax.axis_index("rank")
    y, x = v // 2, v % 2
    z, core = r // 2, r % 2
    vx, vy, vd = y * 2 + 1 - x, (1 - y) * 2 + x, (1 - y) * 2 + 1 - x
    mate = z * 2 + 1 - core
    pairs, rows, cols = acc.shape
    depth = own_ref.shape[1]

    def rank_at(k):
        return ((z + k) % zs) * 2 + core

    barrier = pltpu.get_barrier_semaphore()
    peers = [(v, rank_at(k)) for k in range(1, zs)] + [(vx, r), (vy, r), (v, mate)]
    for peer in peers:
        pl.semaphore_signal(barrier, inc=1, device_id=peer, device_id_type=pl.DeviceIdType.MESH)
    pl.semaphore_wait(barrier, len(peers))

    started = []

    def send(src, rr, vv, sem, to):
        copy = pltpu.make_async_remote_copy(
            src_ref=src,
            dst_ref=gath_ref.at[rr, vv],
            send_sem=sem,
            recv_sem=recv.at[rr, vv],
            device_id=to,
            device_id_type=pl.DeviceIdType.MESH,
        )
        copy.start()
        started.append(copy)

    def arrived(rr, vv):
        pltpu.make_async_copy(gath_ref.at[rr, vv], gath_ref.at[rr, vv], recv.at[rr, vv]).wait()

    send(own_ref, r, v, s2.at[0, 0], (vx, r))
    send(own_ref, r, v, s2.at[0, 1], (vy, r))
    for k in range(1, zs):
        send(own_ref, r, v, s1.at[k], (v, rank_at(k)))
    send(own_ref, r, v, s3.at[0, 0], (v, mate))

    def spread(k):
        rr = rank_at(k)
        arrived(rr, v)
        shard = gath_ref.at[rr, v]
        send(shard, rr, v, s2.at[k, 0], (vx, r))
        send(shard, rr, v, s2.at[k, 1], (vy, r))
        send(shard, rr, v, s3.at[k, 0], (v, mate))

    def relay(k):
        rr = rank_at(k)
        odd = (rr // 2) % 2
        arrived(rr, vx)
        arrived(rr, vy)
        via = (y + odd * (1 - 2 * y)) * 2 + x + (1 - odd) * (1 - 2 * x)
        to = (y + (1 - odd) * (1 - 2 * y)) * 2 + x + odd * (1 - 2 * x)
        send(gath_ref.at[rr, via], rr, via, s2.at[k, 2], (to, r))
        send(gath_ref.at[rr, vx], rr, vx, s3.at[k, 1], (v, mate))
        send(gath_ref.at[rr, vy], rr, vy, s3.at[k, 2], (v, mate))

    def finish(k):
        rr = rank_at(k)
        arrived(rr, vd)
        send(gath_ref.at[rr, vd], rr, vd, s3.at[k, 3], (v, mate))

    def compute(slot, rr, first, tasks=()):
        start = pl.multiple_of(rr * depth, depth)

        @pl.loop(0, depth // 128)
        def _(c):
            piece = fbuf[slot, :, :, pl.ds(pl.multiple_of(c * 128, 128), 128)].reshape(rows, 128)
            fturn[pl.ds(pl.multiple_of(c * 128, 128), 128), :] = piece.T

        def one(i):
            half = half_ref[:, i].reshape(rows, cols)
            coupled = jnp.dot(fturn[...], half, preferred_element_type=jnp.float32)
            weight = kern_ref[pl.ds(start, depth), :].astype(jnp.float32)
            weighted = (weight * coupled).astype(jnp.bfloat16)
            term = jnp.dot(
                fbuf[slot].reshape(rows, depth), weighted, preferred_element_type=jnp.float32
            )
            if first:
                acc[i] = term
            else:
                acc[i] += term

        pieces = 4
        each = pairs // pieces
        for piece in range(pieces):
            if piece < len(tasks):
                tasks[piece]()
            pl.loop(piece * each, (piece + 1) * each)(one)

    def fetch(slot, rr):
        for j in range(4):
            pltpu.make_async_copy(gath_ref.at[rr, j], fbuf.at[slot, j], load_sem.at[slot, j]).start()

    def fetched(slot, rr):
        for j in range(4):
            pltpu.make_async_copy(gath_ref.at[rr, j], fbuf.at[slot, j], load_sem.at[slot, j]).wait()

    stage = fbuf.at[1, 0]
    into = pltpu.make_async_copy(own_ref, stage, mine_sem.at[0])
    into.start()
    into.wait()
    back = pltpu.make_async_copy(stage, gath_ref.at[r, v], mine_sem.at[1])
    back.start()
    back.wait()

    relay(0)
    spread(1)
    finish(0)
    fetch(0, r)
    queue = []
    for k in range(1, zs):
        if k + 1 < zs:
            queue.append(functools.partial(spread, k + 1))
        queue.append(functools.partial(relay, k))
        queue.append(functools.partial(finish, k))
    fetched(0, r)
    compute(0, r, True, queue[:4])
    queue = queue[4:]
    for k in range(zs):
        other = ((z + k) % zs) * 2 + 1 - core
        for at in (v, vx, vy, vd):
            arrived(other, at)
        fetch(1, other)
        if k + 1 < zs:
            fetch(0, rank_at(k + 1))
        fetched(1, other)
        compute(1, other, False, queue[:4])
        queue = queue[4:]
        if k + 1 < zs:
            fetched(0, rank_at(k + 1))
            compute(0, rank_at(k + 1), False, queue[:4])
            queue = queue[4:]
    for i in range(pairs):
        out_ref[:, i] = acc[i].reshape(4, rows // 4, cols).astype(jnp.bfloat16)
    for copy in started:
        copy.wait_send()


def front_kernel(zs, own_ref, amp_ref, cols_ref, amps_ref, mine_sem, cols_recv, amps_recv, cs, us, ds, ms, stage, hold):
    v = lax.axis_index("vpair")
    r = lax.axis_index("rank")
    y, x = v // 2, v % 2
    z, core = r // 2, r % 2
    near = (y * 2 + 1 - x, (1 - y) * 2 + x, (1 - y) * 2 + 1 - x)
    mate = z * 2 + 1 - core
    mesh_ids = pl.DeviceIdType.MESH
    has_up, has_down = z + 1 < zs, z >= 1
    up_to, down_to = ((z + 1) % zs) * 2 + core, ((z + zs - 1) % zs) * 2 + core

    barrier = pltpu.get_barrier_semaphore()
    peers = [(at, r) for at in near] + [(v, mate), (v, up_to), (v, down_to)]
    for peer in peers:
        pl.semaphore_signal(barrier, inc=1, device_id=peer, device_id_type=mesh_ids)
    pl.semaphore_wait(barrier, len(peers))

    def cols_copy(j, at, to):
        return pltpu.make_async_remote_copy(
            src_ref=own_ref, dst_ref=cols_ref.at[at], send_sem=cs.at[j], recv_sem=cols_recv.at[at],
            device_id=(to, r), device_id_type=mesh_ids,
        )

    def amps_copy(src, at, sem, to):
        return pltpu.make_async_remote_copy(
            src_ref=src, dst_ref=amps_ref.at[at], send_sem=sem, recv_sem=amps_recv.at[at],
            device_id=(v, to), device_id_type=mesh_ids,
        )

    def amps_wait(at):
        pltpu.make_async_copy(amps_ref.at[at], amps_ref.at[at], amps_recv.at[at]).wait()

    @pl.when(has_up)
    def _():
        amps_copy(amp_ref, r, us.at[0], up_to).start()

    @pl.when(has_down)
    def _():
        amps_copy(amp_ref, r, ds.at[0], down_to).start()

    for j in range(3):
        cols_copy(j, v, near[j]).start()
    amps_copy(amp_ref, r, ms.at[0, 0], mate).start()
    a = pltpu.make_async_copy(own_ref, stage, mine_sem.at[0])
    b = pltpu.make_async_copy(amp_ref, hold, mine_sem.at[1])
    a.start()
    b.start()
    a.wait()
    b.wait()
    c = pltpu.make_async_copy(stage, cols_ref.at[v], mine_sem.at[2])
    d = pltpu.make_async_copy(hold, amps_ref.at[r], mine_sem.at[3])
    c.start()
    d.start()
    c.wait()
    d.wait()

    for s in range(1, zs):
        low, high = ((z + zs - s) % zs) * 2 + core, ((z + s) % zs) * 2 + core

        @pl.when(z >= s)
        def _():
            amps_wait(low)
            amps_copy(amps_ref.at[low], low, ms.at[s, 0], mate).start()

            @pl.when(has_up)
            def _():
                amps_copy(amps_ref.at[low], low, us.at[s], up_to).start()

        @pl.when(z + s < zs)
        def _():
            amps_wait(high)
            amps_copy(amps_ref.at[high], high, ms.at[s, 1], mate).start()

            @pl.when(has_down)
            def _():
                amps_copy(amps_ref.at[high], high, ds.at[s], down_to).start()

    for at in near:
        pltpu.make_async_copy(cols_ref.at[at], cols_ref.at[at], cols_recv.at[at]).wait()
    for k in range(zs):
        amps_wait(k * 2 + 1 - core)
    for j in range(3):
        cols_copy(j, v, near[j]).wait_send()
    amps_copy(amp_ref, r, ms.at[0, 0], mate).wait_send()
    for s in range(zs):

        @pl.when(jnp.logical_and(z >= s, has_up))
        def _():
            amps_copy(amp_ref, r, us.at[s], up_to).wait_send()

        @pl.when(jnp.logical_and(z + s < zs, has_down))
        def _():
            amps_copy(amp_ref, r, ds.at[s], down_to).wait_send()

        if s:

            @pl.when(z >= s)
            def _():
                amps_copy(amp_ref, r, ms.at[s, 0], mate).wait_send()

            @pl.when(z + s < zs)
            def _():
                amps_copy(amp_ref, r, ms.at[s, 1], mate).wait_send()


def front_gather(factors_pad, amps_pad, vpair_count, rank_count):
    zs = rank_count // 2
    hbm = pl.BlockSpec(memory_space=pl.ANY)
    return pl.pallas_call(
        functools.partial(front_kernel, zs),
        out_shape=(
            jax.ShapeDtypeStruct((vpair_count, *factors_pad.shape), jnp.bfloat16),
            jax.ShapeDtypeStruct((rank_count, *amps_pad.shape), jnp.bfloat16),
        ),
        in_specs=[hbm, hbm],
        out_specs=(hbm, hbm),
        scratch_shapes=[
            pltpu.SemaphoreType.DMA((4,)),
            pltpu.SemaphoreType.DMA((vpair_count,)),
            pltpu.SemaphoreType.DMA((rank_count,)),
            pltpu.SemaphoreType.DMA((3,)),
            pltpu.SemaphoreType.DMA((zs,)),
            pltpu.SemaphoreType.DMA((zs,)),
            pltpu.SemaphoreType.DMA((zs, 2)),
            pltpu.VMEM(factors_pad.shape, jnp.bfloat16),
            pltpu.VMEM(amps_pad.shape, jnp.bfloat16),
        ],
        compiler_params=pltpu.CompilerParams(
            collective_id=1, has_side_effects=True, vmem_limit_bytes=60 * 1024 * 1024
        ),
        cost_estimate=pl.CostEstimate(flops=10**10, bytes_accessed=10**7, transcendentals=0),
    )(factors_pad, amps_pad)


def ladder_middle(factors_pad, half_sub, kernel_sub, rank_count):
    count, pairs, block, cols = half_sub.shape
    depth = factors_pad.shape[1]
    rows = count * block
    points = kernel_sub.shape[0]
    zs = rank_count // 2
    hbm = pl.BlockSpec(memory_space=pl.ANY)
    vmem = pl.BlockSpec(memory_space=pltpu.VMEM)
    return pl.pallas_call(
        functools.partial(middle_kernel, zs),
        out_shape=(
            jax.ShapeDtypeStruct((count, pairs, block, cols), jnp.bfloat16),
            jax.ShapeDtypeStruct((rank_count, count, block, depth), jnp.bfloat16),
        ),
        in_specs=[hbm, vmem, vmem],
        out_specs=(vmem, hbm),
        scratch_shapes=[
            pltpu.VMEM((2, count, block, depth), jnp.bfloat16),
            pltpu.VMEM((depth, rows), jnp.bfloat16),
            pltpu.VMEM((pairs, rows, cols), jnp.float32),
            pltpu.SemaphoreType.DMA((2,)),
            pltpu.SemaphoreType.DMA((2, count)),
            pltpu.SemaphoreType.DMA((rank_count, count)),
            pltpu.SemaphoreType.DMA((zs,)),
            pltpu.SemaphoreType.DMA((zs, 3)),
            pltpu.SemaphoreType.DMA((zs, 4)),
        ],
        compiler_params=pltpu.CompilerParams(
            collective_id=0, has_side_effects=True, vmem_limit_bytes=60 * 1024 * 1024
        ),
        cost_estimate=pl.CostEstimate(
            flops=4 * pairs * points * rows * cols, bytes_accessed=4 * points * rows, transcendentals=0
        ),
    )(factors_pad, half_sub, kernel_sub)


def fast_shards(amplitudes, factors, kernel, other_terms, virt_energy, pair_energy):
    vpair_count = lax.axis_size("vpair")
    rank_count = lax.axis_size("rank")
    pair_count, row_block, _ = amplitudes.shape
    virt_count = row_block * vpair_count
    right_block = kernel.shape[1]
    cols = right_block // vpair_count
    block = -(-row_block // 64) * 64
    col_block = amplitudes.shape[2]
    deep = -(-col_block // 16) * 16
    kernel_sub = lax.all_to_all(kernel, "vpair", split_axis=1, concat_axis=0, tiled=True)
    factors_pad = jnp.pad(factors, ((0, block - row_block), (0, 0)))
    amps_pad = jnp.pad(
        amplitudes.transpose(2, 0, 1), ((0, deep - col_block), (0, 0), (0, block - row_block))
    ).reshape(deep, pair_count * block)
    cols_pad, amps = front_gather(factors_pad, amps_pad, vpair_count, rank_count)
    factor_cols = cols_pad[:, :row_block].reshape(virt_count, right_block)
    cols_deep = jnp.pad(
        factor_cols.reshape(rank_count, col_block, right_block), ((0, 0), (0, deep - col_block), (0, 0))
    ).reshape(rank_count * deep, right_block)
    half_done = jnp.einsum(
        "sm,sh->mh",
        amps.reshape(rank_count * deep, pair_count * block),
        cols_deep,
        preferred_element_type=jnp.float32,
    ).astype(jnp.bfloat16)
    half_done = half_done.reshape(pair_count, block, vpair_count, cols).transpose(2, 0, 1, 3)
    half_sub = lax.all_to_all(half_done, "vpair", split_axis=0, concat_axis=0, tiled=True)
    back, _ = ladder_middle(factors_pad, half_sub, kernel_sub, rank_count)
    back = lax.all_to_all(back, "vpair", split_axis=0, concat_axis=0, tiled=True)
    back = back[:, :, :row_block]
    partial_value = jnp.einsum(
        "viaq,bvq->iab",
        back,
        factor_cols.reshape(virt_count, vpair_count, cols),
        preferred_element_type=jnp.float32,
    )
    ladder_own = lax.psum_scatter(partial_value, "rank", scatter_dimension=0, tiled=True)
    ladder = lax.all_gather(ladder_own.astype(jnp.bfloat16), "rank", axis=0, tiled=True)
    own = ladder_own.shape[0]
    start = lax.axis_index("rank") * own
    row_energy = lax.dynamic_slice_in_dim(
        virt_energy, lax.axis_index("vpair") * row_block, row_block, 0
    )
    own_terms = lax.optimization_barrier(lax.dynamic_slice_in_dim(other_terms, start, own, 0))
    own_pairs = lax.dynamic_slice_in_dim(pair_energy, start, own, 0)
    denominator = row_energy[None, :, None] + virt_energy[None, None, :] - own_pairs[:, None, None]
    update = (own_terms + ladder_own) / denominator
    squares = lax.psum(jnp.sum(update * update), ("vpair", "rank"))
    squares, ladder = lax.optimization_barrier((squares, ladder))
    turned = lax.optimization_barrier(ladder.transpose(1, 0, 2))
    residual = (other_terms.transpose(1, 0, 2) + turned.astype(jnp.float32)).transpose(1, 0, 2)
    update_rms = jnp.sqrt(squares / (pair_count * virt_count * virt_count) + epsilon)
    return (residual, update_rms)


def pick(amplitudes, factors, kernel, other_terms, virt_energy, pair_energy):
    vpair_count = lax.axis_size("vpair")
    rank_count = lax.axis_size("rank")
    fits = (
        vpair_count == 4
        and rank_count % 2 == 0
        and amplitudes.shape[0] % rank_count == 0
        and kernel.shape[1] % (128 * vpair_count) == 0
    )
    body = fast_shards if fits else shards
    return body(amplitudes, factors, kernel, other_terms, virt_energy, pair_energy)


def solution(mesh):
    placed = (
        P(None, "vpair", "rank"),
        P("vpair", "rank"),
        P("vpair", "rank"),
        P(None, "vpair", None),
        P(),
        P(),
    )
    return jax.shard_map(
        pick, mesh=mesh, in_specs=placed, out_specs=(P(None, "vpair", None), P()), check_vma=False
    )
```
